32 devices in a mesh: doc: 8 (over y, x, core), seg: 4 (over z).
Axes of the slice: x: 2, y: 2, z: 4, core: 2. Of those that a mesh axis runs over, the one named last changes fastest.
Arguments:
- tokens: int32 [2048], P(('doc', 'seg')), parts along dimension 0, may hold values from 0 to 20479
- targets: int32 [2048], P(('doc', 'seg')), parts along dimension 0, may hold values from 0 to 20479
- embedding: bfloat16 [20480, 1024], P('seg'), may hold values from -2 to 2
- qkv_weight: bfloat16 [2, 1024, 3, 1024], P(None, None, None, 'seg'), may hold values from -2 to 2
- pos_weight: bfloat16 [2, 1024, 1024], P(None, None, 'seg'), may hold values from -0.375 to 0.375
- out_weight: bfloat16 [2, 1024, 1024], P(None, None, 'seg'), may hold values from -0.1875 to 0.1875
- content_bias: float32 [2, 1024], replicated, may hold values from -3 to 3
- position_bias: float32 [2, 1024], replicated, may hold values from -6 to 6
- norm_gain: float32 [2, 1024], replicated, may hold values from 0.25 to 8
- norm_shift: float32 [2, 1024], replicated, may hold values from -2 to 2
Outputs:
- token_loglik: float32 [2048], P(('doc', 'seg')), parts along dimension 0
- doc_mean: float32 [8], P('doc'), parts along dimension 0
The draws below stay inside these ranges and needn't reach their ends.
There are 8 independent parts, one for each index of `doc`. The reference program is written for one: setup_inputs(seed, part) draws one part's arguments, and reference() takes and returns one part's arrays. A program takes and returns all parts, laid end to end along the dimension named above; an argument that names none is the same for every part. Nothing has to cross between parts.
All inputs are finite; a program needn't handle non-finite values.
Results may differ from the reference program's by a relative error of at most 0.005.
The reference program's roundings to bfloat16 on the way (of `hidden`, `pos_table`, `project`, `pos_keys`, `keys_all`, `attn_probs` and `head_mix`) count: a program that leaves them out, or rounds other values in their place, can miss the bound.
Values may be sent and summed in bfloat16 or wider, within the bound.
A program may use at most 128 MiB of HBM per device.

```python
import math
import jax
import jax.numpy as jnp
import numpy as np
from jax import lax

D = 1024
HEADS = 16
SEG = 64
MEM_SEGS = 6
LAYERS = 2
VOCAB = 20480
TOKENS = 256


def draw_embedding(key, part):
    own_key = jax.random.fold_in(key, 11)
    values = jnp.clip(jax.random.normal(own_key, (VOCAB, D), jnp.float32), -6.0, 6.0) / 32.0
    return values.astype(jnp.bfloat16)


def draw_qkv_weight(key, part):
    own_key = jax.random.fold_in(key, 13)
    values = jnp.clip(jax.random.normal(own_key, (LAYERS, D, 3, D), jnp.float32), -6.0, 6.0) / math.sqrt(D)
    return values.astype(jnp.bfloat16)


def draw_norm_gain(key, part):
    own_key = jax.random.fold_in(key, 12)
    return jax.random.uniform(own_key, (LAYERS, D), jnp.float32, 0.8, 1.2)


def with_ends(result, stream_key, low, largest):
    longest = result.shape.index(max(result.shape))
    spots = []
    for shift in (0, 1):
        where = [jax.random.randint(jax.random.fold_in(stream_key, axis), (), 0, length) for axis, length in enumerate(result.shape)]
        where[longest] = (where[longest] + shift) % result.shape[longest]
        spots.append(tuple(where))
    return result.at[spots[0]].set(low).at[spots[1]].set(largest)


def level_of(key, dims, shards, low, largest):
    loudness = 1.0
    for position, blocks in shards:
        draws = jax.random.uniform(jax.random.fold_in(jax.random.fold_in(key, 6), position), (blocks,), jnp.float32, low / len(shards), largest / len(shards))
        loudness = loudness * jnp.repeat(jnp.exp(draws), dims[position] // blocks).reshape((-1,) + (1,) * (len(dims) - 1 - position))
    return loudness


def cumulative_ranks(amount, lean):
    weights = [(1 << 20) // math.isqrt(standing ** lean) + 1 for standing in range(1, amount + 1)]
    deviation = 1 + sum(weights) // (1 << 30)
    return np.cumsum(np.array([max(1, weight // deviation) for weight in weights]))


def ranked_ids(stream_key, dims, count, skew):
    grid = cumulative_ranks(count, skew)
    ticket = jax.random.randint(jax.random.fold_in(stream_key, 1), dims, 0, int(grid[count - 1]))
    grade = jnp.searchsorted(jnp.asarray(grid, jnp.int32), ticket, side="right")
    return jax.random.permutation(jax.random.fold_in(stream_key, 2), count)[grade].astype(jnp.int32)


def scatter_about(stream_key, dims, scale, reach, cuts=(), held_as=jnp.bfloat16):
    drawn = scale * jax.random.normal(stream_key, dims, jnp.float32)
    if cuts:
        drawn = drawn * level_of(stream_key, dims, cuts, -0.22, 0.18)
    return jnp.clip(drawn, -reach, reach).astype(held_as)


def setup_inputs(seed: int = 0, part: int = 0) -> dict:
    arg_keys = jax.random.split(jax.random.key(seed), 11)
    part_keys = jax.random.split(jax.random.fold_in(arg_keys[10], part), 11)
    tokens = with_ends(ranked_ids(part_keys[0], (TOKENS,), VOCAB, 2), jax.random.fold_in(part_keys[0], 3), 0, VOCAB - 1).astype(jnp.int32)
    targets = with_ends(ranked_ids(part_keys[1], (TOKENS,), VOCAB, 2), jax.random.fold_in(part_keys[1], 3), 0, VOCAB - 1).astype(jnp.int32)
    embedding = draw_embedding(jax.random.fold_in(arg_keys[10], 71), part)
    qkv_weight = draw_qkv_weight(jax.random.fold_in(arg_keys[10], 71), part)
    pos_weight = scatter_about(arg_keys[4], (LAYERS, D, D), (D // 4) ** -0.5, 0.375, ((2, 4),))
    out_weight = scatter_about(arg_keys[5], (LAYERS, D, D), D ** -0.5, 0.1875, ((2, 4),))
    content_bias = scatter_about(arg_keys[6], (LAYERS, D), 0.5, 3.0, (), jnp.float32)
    position_bias = scatter_about(arg_keys[7], (LAYERS, D), 1.5, 6.0, (), jnp.float32)
    norm_gain = draw_norm_gain(jax.random.fold_in(arg_keys[10], 71), part)
    norm_shift = scatter_about(arg_keys[9], (LAYERS, D), 0.3, 2.0, (), jnp.float32)
    return dict(tokens=tokens, targets=targets, embedding=embedding, qkv_weight=qkv_weight, pos_weight=pos_weight, out_weight=out_weight, content_bias=content_bias, position_bias=position_bias, norm_gain=norm_gain, norm_shift=norm_shift)


def layer_norm(total, gain, shift):
    middle = lax.optimization_barrier(jnp.mean(total, axis=-1, keepdims=True))
    spread = lax.optimization_barrier(jnp.mean(jnp.square(total - middle), axis=-1, keepdims=True))
    return ((total - middle) / jnp.sqrt(spread + 1e-05) * gain + shift).astype(jnp.bfloat16)

def position_table(key_len, model_width):
    places = (key_len - 1 - jnp.arange(key_len)).astype(jnp.float32)
    inverse = jnp.power(10000.0, -jnp.arange(0, model_width, 2).astype(jnp.float32) / model_width)
    angles = places[:, None] * inverse[None, :]
    return jnp.concatenate([jnp.sin(angles), jnp.cos(angles)], axis=1).astype(jnp.bfloat16)

def reference(tokens, targets, embedding, qkv_weight, pos_weight, out_weight, content_bias, position_bias, norm_gain, norm_shift):
    mem_len = MEM_SEGS * SEG
    key_len = mem_len + SEG
    head_dim = D // HEADS
    seg_count = TOKENS // SEG
    pos_table = position_table(key_len, D)
    hidden = (embedding[tokens].astype(jnp.float32) * math.sqrt(D)).astype(jnp.bfloat16)
    row_ids = jnp.arange(SEG)[:, None]
    col_ids = jnp.arange(key_len)[None, :]
    shift_ids = jnp.clip(col_ids + SEG - 1 - row_ids, 0, key_len - 1)
    shift_ids = jnp.broadcast_to(shift_ids[None], (HEADS, SEG, key_len))
    for layer_at in range(LAYERS):
        layer_qkv = qkv_weight[layer_at].reshape(D, 3 * D)
        project = jnp.dot(hidden, layer_qkv, preferred_element_type=jnp.float32).astype(jnp.bfloat16)
        pos_keys = jnp.dot(pos_table, pos_weight[layer_at], preferred_element_type=jnp.float32).astype(jnp.bfloat16)
        padded_kv = jnp.concatenate([jnp.zeros((mem_len, 2 * D), jnp.bfloat16), project[:, D:]], axis=0)
        pos_heads = pos_keys.reshape(key_len, HEADS, head_dim).astype(jnp.float32)
        u_bias = content_bias[layer_at]
        v_bias = position_bias[layer_at]

        def one_segment(seg_at):
            start = (seg_at * SEG).astype(jnp.int32)
            own = lax.dynamic_slice_in_dim(project, start, SEG, 0)
            keys_all = lax.dynamic_slice_in_dim(padded_kv, start, key_len, 0)
            queries = own[:, :D].astype(jnp.float32)
            with_content = (queries + u_bias).astype(jnp.bfloat16).reshape(SEG, HEADS, head_dim)
            with_position = (queries + v_bias).astype(jnp.bfloat16).reshape(SEG, HEADS, head_dim)
            key_heads = keys_all[:, :D].reshape(key_len, HEADS, head_dim)
            value_heads = keys_all[:, D:].reshape(key_len, HEADS, head_dim)
            content = jnp.einsum('thd,khd->htk', with_content.astype(jnp.float32), key_heads.astype(jnp.float32))
            raw_position = jnp.einsum('thd,khd->htk', with_position.astype(jnp.float32), pos_heads)
            shifted = jnp.take_along_axis(raw_position, shift_ids, axis=2)
            scores = (content + shifted) * (1.0 / math.sqrt(head_dim))
            visible = (col_ids <= row_ids + mem_len) & (col_ids >= mem_len - seg_at * SEG)
            scores = jnp.where(visible[None], scores, jnp.float32(-1e+30))
            row_max = lax.optimization_barrier(jnp.max(scores, axis=2, keepdims=True))
            weights = jnp.exp(scores - row_max)
            attn_probs = (weights / lax.optimization_barrier(jnp.sum(weights, axis=2, keepdims=True))).astype(jnp.bfloat16)
            head_mix = jnp.einsum('htk,khd->thd', attn_probs.astype(jnp.float32), value_heads.astype(jnp.float32))
            return head_mix.astype(jnp.bfloat16).reshape(SEG, D)
        head_mix = lax.map(one_segment, jnp.arange(seg_count).astype(jnp.int32)).reshape(TOKENS, D)
        attended = jnp.dot(head_mix, out_weight[layer_at], preferred_element_type=jnp.float32)
        hidden = layer_norm(hidden.astype(jnp.float32) + attended, norm_gain[layer_at], norm_shift[layer_at])

    def segment_loglik(seg_at):
        start = (seg_at * SEG).astype(jnp.int32)
        rows = lax.dynamic_slice_in_dim(hidden, start, SEG, 0)
        wanted = lax.dynamic_slice_in_dim(targets.astype(jnp.int32), start, SEG, 0)
        logits = jnp.dot(rows, embedding.T, preferred_element_type=jnp.float32)
        row_max = lax.optimization_barrier(jnp.max(logits, axis=1, keepdims=True))
        log_total = jnp.log(lax.optimization_barrier(jnp.sum(jnp.exp(logits - row_max), axis=1))) + row_max[:, 0]
        picked = jnp.take_along_axis(logits, wanted[:, None].astype(jnp.int32), axis=1)[:, 0]
        return picked - log_total
    token_loglik = lax.map(segment_loglik, jnp.arange(seg_count).astype(jnp.int32)).reshape(TOKENS)
    doc_mean = (jnp.sum(token_loglik) / TOKENS).reshape(1)
    return (token_loglik, doc_mean)
```

```python
import functools
import math

import jax
import jax.numpy as jnp
from jax import lax
from jax.experimental import pallas as pl
from jax.experimental.pallas import tpu as pltpu
from jax.sharding import PartitionSpec as P

HEADS = 16
MEM_SEGS = 6
LAYERS = 2


def merged(shard, axis, combine):
    everything = jax.tree.map(lambda part: lax.all_gather(part, axis), shard)
    initial = jax.tree.map(lambda part: part[0], everything)

    def hop(k, so_far):
        return combine(so_far, jax.tree.map(lambda part: part[k], everything))

    return lax.fori_loop(1, lax.axis_size(axis), hop, initial)


def layer_norm(total, gain, shift):
    middle = jnp.mean(total, axis=-1, keepdims=True)
    spread = jnp.mean(jnp.square(total - middle), axis=-1, keepdims=True)
    return ((total - middle) / jnp.sqrt(spread + 1e-05) * gain + shift).astype(jnp.bfloat16)


def position_table(key_len, model_width):
    places = (key_len - 1 - jnp.arange(key_len)).astype(jnp.float32)
    inverse = jnp.power(10000.0, -jnp.arange(0, model_width, 2).astype(jnp.float32) / model_width)
    angles = places[:, None] * inverse[None, :]
    return jnp.concatenate([jnp.sin(angles), jnp.cos(angles)], axis=1).astype(jnp.bfloat16)


def relative_shift(raw_position, query_len, key_len):
    head_count = raw_position.shape[0]
    padded = jnp.pad(raw_position, ((0, 0), (0, 0), (0, 1)))
    flattened = padded.reshape(head_count, query_len * (key_len + 1))
    shifted = lax.slice_in_dim(
        flattened, query_len - 1, query_len - 1 + query_len * key_len, axis=1
    )
    return shifted.reshape(head_count, query_len, key_len)


def attend(with_content, with_position, key_heads, value_heads, pos_heads, visible, head_dim):
    query_len = with_content.shape[0]
    key_len = key_heads.shape[0]
    content = jnp.einsum(
        "thd,khd->htk", with_content, key_heads, preferred_element_type=jnp.float32
    )
    raw_position = jnp.einsum(
        "thd,khd->htk", with_position, pos_heads, preferred_element_type=jnp.float32
    )
    shifted = relative_shift(raw_position, query_len, key_len)
    scores = (content + shifted) * (1.0 / math.sqrt(head_dim))
    scores = jnp.where(visible[None], scores, jnp.float32(-1e30))
    row_max = jnp.max(scores, axis=2, keepdims=True)
    weights = jnp.exp(scores - row_max)
    attn_probs = (weights / jnp.sum(weights, axis=2, keepdims=True)).astype(jnp.bfloat16)
    head_mix = jnp.einsum(
        "htk,khd->thd", attn_probs, value_heads, preferred_element_type=jnp.float32
    )
    return head_mix.astype(jnp.bfloat16).reshape(query_len, with_content.shape[1] * head_dim)


def head_attention(layer_input, qkv_local, pos_local, u_row, v_row, head_dim):
    seg_len = layer_input.shape[0]
    model_width = layer_input.shape[1]
    group_size = lax.axis_size("seg")
    columns = qkv_local.shape[2]
    head_count = columns // head_dim
    mem_len = MEM_SEGS * seg_len
    first_column = lax.axis_index("seg") * columns
    matrix = qkv_local.reshape(model_width, 3 * columns)
    piece = lax.all_gather(layer_input, "seg", axis=0, tiled=True)
    product = jnp.dot(piece, matrix, preferred_element_type=jnp.float32)
    project = product.astype(jnp.bfloat16).reshape(piece.shape[0], 3, columns)
    total_rows = project.shape[0]
    block_segs = min(group_size, max(1, 512 // seg_len))
    while group_size % block_segs != 0:
        block_segs -= 1
    block_len = block_segs * seg_len
    key_span = mem_len + block_len
    block_count = group_size // block_segs
    pos_table = position_table(key_span, model_width)
    pos_keys = jnp.dot(pos_table, pos_local, preferred_element_type=jnp.float32).astype(
        jnp.bfloat16
    )
    pos_heads = pos_keys.reshape(key_span, head_count, head_dim)
    queries = project[:, 0, :].astype(jnp.float32)
    u_part = lax.dynamic_slice_in_dim(u_row, first_column, columns, 0)
    v_part = lax.dynamic_slice_in_dim(v_row, first_column, columns, 0)
    with_content = (queries + u_part).astype(jnp.bfloat16).reshape(total_rows, head_count, head_dim)
    with_position = (
        (queries + v_part).astype(jnp.bfloat16).reshape(total_rows, head_count, head_dim)
    )
    padded_kv = jnp.concatenate(
        [jnp.zeros((mem_len, 2, columns), jnp.bfloat16), project[:, 1:, :]], axis=0
    )
    row_ids = jnp.arange(block_len)[:, None]
    col_ids = jnp.arange(key_span)[None, :]

    def one_block(block_at):
        start = block_at * block_len
        block_content = lax.dynamic_slice_in_dim(with_content, start, block_len, 0)
        block_position = lax.dynamic_slice_in_dim(with_position, start, block_len, 0)
        window = lax.dynamic_slice_in_dim(padded_kv, start, key_span, 0)
        key_heads = window[:, 0, :].reshape(key_span, head_count, head_dim)
        value_heads = window[:, 1, :].reshape(key_span, head_count, head_dim)
        query_place = start + row_ids
        key_place = start - mem_len + col_ids
        visible = (key_place <= query_place) & (key_place >= 0)
        visible = visible & (key_place >= query_place // seg_len * seg_len - mem_len)
        return attend(
            block_content, block_position, key_heads, value_heads, pos_heads, visible, head_dim
        )

    mixed = lax.map(one_block, jnp.arange(block_count, dtype=jnp.int32)).reshape(
        total_rows, columns
    )
    return lax.all_to_all(mixed, "seg", split_axis=0, concat_axis=1, tiled=True)


def combine_words(first, second):
    top = jnp.maximum(first[0], second[0])
    total = first[1] * jnp.exp(first[0] - top) + second[1] * jnp.exp(second[0] - top)
    return (top, total, first[2] + second[2])


def on_device(
    tokens,
    targets,
    embedding,
    qkv_weight,
    pos_weight,
    out_weight,
    content_bias,
    position_bias,
    norm_gain,
    norm_shift,
):
    seg_len = tokens.shape[0]
    model_width = embedding.shape[1]
    vocab_rows = embedding.shape[0]
    head_dim = model_width // HEADS
    seg_index = lax.axis_index("seg")
    group_size = lax.axis_size("seg")
    first_word = seg_index * vocab_rows
    all_tokens, all_targets = (
        lax.all_gather(tokens, "seg", axis=0, tiled=True),
        lax.all_gather(targets, "seg", axis=0, tiled=True),
    )
    local_ids = all_tokens - first_word
    inside = (local_ids >= 0) & (local_ids < vocab_rows)
    rows = jnp.take(embedding, jnp.clip(local_ids, 0, vocab_rows - 1), axis=0)
    looked = lax.psum_scatter(
        jnp.where(inside[:, None], rows.astype(jnp.float32), 0.0).astype(jnp.bfloat16),
        "seg",
        scatter_dimension=0,
        tiled=True,
    ).astype(jnp.float32)
    hidden = (looked * math.sqrt(model_width)).astype(jnp.bfloat16)
    for layer_at in range(LAYERS):
        layer_input = hidden
        head_mix = head_attention(
            layer_input,
            qkv_weight[layer_at],
            pos_weight[layer_at],
            content_bias[layer_at],
            position_bias[layer_at],
            head_dim,
        )
        attended = jnp.dot(
            head_mix,
            lax.all_gather(out_weight[layer_at], "seg", axis=1, tiled=True),
            preferred_element_type=jnp.float32,
        )
        hidden = layer_norm(
            layer_input.astype(jnp.float32) + attended, norm_gain[layer_at], norm_shift[layer_at]
        )
    word_ids = first_word + jnp.arange(vocab_rows)[None, :]
    logits = jnp.einsum(
        "td,vd->tv",
        lax.all_gather(hidden, "seg", axis=0, tiled=True),
        embedding,
        preferred_element_type=jnp.float32,
    )
    piece_max = jnp.max(logits, axis=1)
    piece_sum = jnp.sum(jnp.exp(logits - piece_max[:, None]), axis=1)
    piece_pick = jnp.sum(jnp.where(word_ids == all_targets[:, None], logits, 0.0), axis=1)
    top, total, picked = merged((piece_max, piece_sum, piece_pick), "seg", combine_words)
    own_start = seg_index * seg_len
    own_top = lax.dynamic_slice_in_dim(top, own_start, seg_len, 0)
    own_total = lax.dynamic_slice_in_dim(total, own_start, seg_len, 0)
    own_pick = lax.dynamic_slice_in_dim(picked, own_start, seg_len, 0)
    token_loglik = own_pick - (jnp.log(own_total) + own_top)
    grand_total = lax.psum(jnp.sum(token_loglik), "seg")
    doc_mean = (grand_total / (seg_len * group_size)).reshape(1)
    return (token_loglik, doc_mean)


MESH = pl.DeviceIdType.MESH
EPS = 1e-05


def mega_kernel(
    n, docs, seg_len, mem_len, head_dim,
    ids_ref, emb_hbm, qkv_hbm, pos_hbm, out_hbm, cb_ref, pb_ref, ng_ref, ns_ref,
    lo_sin, lo_cos, hi_sin, hi_cos,
    row_out, mean_out,
    emb, qkv, posw, wfull, idbuf, onehot, gsend, rsbuf, hid, table, pkeys, mixg, stats, xres,
    emb_sem, w_sem, p_sem, o_sem,
    id_s, id_r, rs_s, rs_r, ag_s, ag_r, w1_s, w1_r, w2_s, w2_r, w3_s, w3_r, mx_s, mx_r, st_s, st_r,
):
    layers = qkv.shape[0]
    total = n * seg_len
    vocab, width = emb.shape
    cols = width // n
    chunks = hid.shape[0]
    cw = hid.shape[2]
    per = width // docs
    me = lax.axis_index("seg")
    doc = lax.axis_index("doc")
    pairs = docs // 2
    core = lax.rem(doc, 2)
    chip = doc // 2
    partner = chip * 2 + 1 - core

    def seg_peer(k):
        return (doc, lax.rem(me + k, n))

    def plane_peer(j):
        return (lax.rem(chip + j, pairs) * 2 + core, me)

    def remote(src, dst, send, recv, device):
        return pltpu.make_async_remote_copy(
            src_ref=src, dst_ref=dst, send_sem=send, recv_sem=recv,
            device_id=device, device_id_type=MESH,
        )

    emb_copies = [
        pltpu.make_async_copy(
            emb_hbm.at[:, c * cw : (c + 1) * cw], emb.at[:, c * cw : (c + 1) * cw], emb_sem.at[c]
        )
        for c in range(chunks)
    ]
    out_copies = [
        pltpu.make_async_copy(out_hbm.at[l], wfull.at[l, me], o_sem.at[l]) for l in range(layers)
    ]
    pos_copy = pltpu.make_async_copy(pos_hbm, posw, p_sem)
    qkv_copy = pltpu.make_async_copy(qkv_hbm, qkv, w_sem)
    out_copies[0].start()
    emb_copies[0].start()
    for copy in emb_copies[1:]:
        copy.start()
    for copy in out_copies[1:]:
        copy.start()
    pos_copy.start()
    qkv_copy.start()

    barrier = pltpu.get_barrier_semaphore()
    friends = [seg_peer(k) for k in range(1, n)] + [plane_peer(j) for j in range(1, pairs)]
    friends.append((partner, me))
    for friend in friends:
        pl.semaphore_signal(barrier, inc=1, device_id=friend, device_id_type=MESH)
    pl.semaphore_wait(barrier, len(friends))

    id_copies = [
        remote(ids_ref, idbuf.at[k - 1], id_s.at[k - 1], id_r.at[k - 1], seg_peer(k))
        for k in range(1, n)
    ]
    for copy in id_copies:
        copy.start()

    mine = pl.ds(pl.multiple_of(doc * per, per), per)

    def w1(l):
        return [
            remote(
                wfull.at[l, me, mine], wfull.at[l, me, mine], w1_s.at[l, k - 1],
                w1_r.at[l, k - 1], seg_peer(k),
            )
            for k in range(1, n)
        ]

    w1_copies = [w1(l) for l in range(layers)]
    out_copies[0].wait()
    for copy in w1_copies[0]:
        copy.start()

    def w2(l):
        found = []
        for k in range(1, n):
            src = lax.rem(me - k + n, n)
            for j in range(1, pairs):
                ref = wfull.at[l, src, mine]
                found.append(
                    remote(ref, ref, w2_s.at[l, k - 1, j - 1], w2_r.at[l, k - 1, j - 1], plane_peer(j))
                )
        return found

    def w3(l):
        found = []
        for k in range(1, n):
            src = lax.rem(me - k + n, n)
            for j in range(pairs):
                owner = lax.rem(chip - j + pairs, pairs) * 2 + core
                ref = wfull.at[l, src, pl.ds(pl.multiple_of(owner * per, per), per)]
                found.append(
                    remote(ref, ref, w3_s.at[l, k - 1, j], w3_r.at[l, k - 1, j], (partner, me))
                )
        return found

    w2_copies = [w2(l) for l in range(layers)]
    w3_copies = [w3(l) for l in range(layers)]

    eye = lax.broadcasted_iota(jnp.int32, (2 * seg_len, 2 * seg_len), 0) == lax.broadcasted_iota(
        jnp.int32, (2 * seg_len, 2 * seg_len), 1
    )

    def column(row):
        return jnp.sum(jnp.where(eye, row, 0), axis=1, keepdims=True)

    for copy in id_copies:
        copy.wait_recv()
    idbuf[n - 1] = ids_ref[...]
    first_word = me * vocab
    tok_cols = []
    tgt_cols = []
    for s in range(n):
        slot = lax.rem(me - s + 2 * n - 1, n)
        both = column(idbuf[slot, 0:1, :]) - first_word
        tok_cols.append(both[:seg_len])
        tgt_cols.append(both[seg_len:])
    tokens = jnp.concatenate(tok_cols, axis=0)
    targets = jnp.concatenate(tgt_cols, axis=0)
    wb = 512
    for v in range(vocab // wb):
        words = lax.broadcasted_iota(jnp.int32, (total, wb), 1) + v * wb
        onehot[:, v * wb : (v + 1) * wb] = (tokens == words).astype(jnp.float32).astype(jnp.bfloat16)

    def rows_of(s):
        return pl.ds(pl.multiple_of(s * seg_len, seg_len), seg_len)

    rs_copies = []
    for c in range(chunks):
        emb_copies[c].wait()
        gsend[c] = jnp.dot(
            onehot[...], emb[:, c * cw : (c + 1) * cw], preferred_element_type=jnp.float32
        ).astype(jnp.bfloat16)
        group = []
        for k in range(1, n):
            peer = lax.rem(me + k, n)
            copy = remote(
                gsend.at[c, rows_of(peer)], rsbuf.at[c, k - 1], rs_s.at[c, k - 1],
                rs_r.at[c, k - 1], (doc, peer),
            )
            copy.start()
            group.append(copy)
        rs_copies.append(group)

    for copy in w1_copies[0]:
        copy.wait_recv()
    for copy in w2_copies[0]:
        copy.start()
    out_copies[1].wait()

    step = lo_sin.shape[0]
    half = width // 2
    for a in range(total // step):
        hs = hi_sin[a : a + 1, :]
        hc = hi_cos[a : a + 1, :]
        rows = slice(a * step, (a + 1) * step)
        table[rows, :half] = (hs * lo_cos[...] + hc * lo_sin[...]).astype(jnp.bfloat16)
        table[rows, half:] = (hc * lo_cos[...] - hs * lo_sin[...]).astype(jnp.bfloat16)

    ag_copies = []
    for c in range(chunks):
        for copy in rs_copies[c]:
            copy.wait_recv()
        own = gsend[c, rows_of(me), :].astype(jnp.float32)
        for k in range(1, n):
            own = own + rsbuf[c, k - 1].astype(jnp.float32)
        hid[c, rows_of(me), :] = (own * math.sqrt(width)).astype(jnp.bfloat16)
        group = []
        for k in range(1, n):
            ref = hid.at[c, rows_of(me)]
            copy = remote(ref, ref, ag_s.at[c, k - 1], ag_r.at[c, k - 1], seg_peer(k))
            copy.start()
            group.append(copy)
        ag_copies.append(group)

    for l in range(1, layers):
        for copy in w1_copies[l]:
            copy.start()

    pos_copy.wait()
    for l in range(layers):
        pkeys[l] = jnp.dot(table[...], posw[l], preferred_element_type=jnp.float32).astype(
            jnp.bfloat16
        )
    for copy in w2_copies[0]:
        copy.wait_recv()
    for copy in w3_copies[0]:
        copy.start()
    qkv_copy.wait()
    for c in range(chunks):
        for copy in ag_copies[c]:
            copy.wait()

    row_ids = lax.broadcasted_iota(jnp.int32, (total, total), 0)
    col_ids = lax.broadcasted_iota(jnp.int32, (total, total), 1)
    seg_start = row_ids // seg_len * seg_len
    visible = (col_ids <= row_ids) & (col_ids >= seg_start - mem_len)
    lanes = lax.broadcasted_iota(jnp.int32, (1, cols), 1) // head_dim
    heads = cols // head_dim
    own_cols = pl.ds(pl.multiple_of(me * cols, cols), cols)
    nt = (((1,), (1,)), ((), ()))
    mx_all = []

    for l in range(layers):
        parts = []
        for j in range(3):
            acc = None
            for c in range(chunks):
                term = jnp.dot(
                    hid[c], qkv[l, c * cw : (c + 1) * cw, j * cols : (j + 1) * cols],
                    preferred_element_type=jnp.float32,
                )
                acc = term if acc is None else acc + term
            parts.append(acc.astype(jnp.bfloat16))
        query, key, value = parts
        query = query.astype(jnp.float32)
        content_q = query + cb_ref[l : l + 1, own_cols]
        position_q = query + pb_ref[l : l + 1, own_cols]
        mixed = jnp.zeros((total, cols), jnp.float32)
        for h in range(heads):
            here = lanes == h
            cq = jnp.where(here, content_q, 0.0).astype(jnp.bfloat16)
            pq = jnp.where(here, position_q, 0.0).astype(jnp.bfloat16)
            content = lax.dot_general(cq, key, nt, preferred_element_type=jnp.float32)
            raw = lax.dot_general(pq, pkeys[l], nt, preferred_element_type=jnp.float32)
            shifted = pltpu.roll(raw, 1, 1, stride=1, stride_axis=0)
            scores = (content + shifted) * (1.0 / math.sqrt(head_dim))
            scores = jnp.where(visible, scores, -1e30)
            top = jnp.max(scores, axis=1, keepdims=True)
            weights = jnp.exp(scores - top)
            probs = (weights * (1.0 / jnp.sum(weights, axis=1, keepdims=True))).astype(jnp.bfloat16)
            out = jnp.dot(probs, value, preferred_element_type=jnp.float32)
            mixed = jnp.where(here, out, mixed)
        mixg[l, me] = mixed.astype(jnp.bfloat16)
        mx = []
        for k in range(1, n):
            ref = mixg.at[l, me]
            copy = remote(ref, ref, mx_s.at[l, k - 1], mx_r.at[l, k - 1], seg_peer(k))
            copy.start()
            mx.append(copy)
        if l + 1 < layers:
            for copy in w1_copies[l + 1]:
                copy.wait_recv()
            for copy in w2_copies[l + 1]:
                copy.start()
        if l > 0:
            for copy in w2_copies[l]:
                copy.wait_recv()
            for copy in w3_copies[l]:
                copy.start()
        for copy in w3_copies[l]:
            copy.wait_recv()
        for copy in mx:
            copy.wait()
        for s in range(n):
            acc = hid_cols(hid, s, cols)
            for k in range(n):
                acc = acc + jnp.dot(
                    mixg[l, k], wfull[l, s, k * cols : (k + 1) * cols, :],
                    preferred_element_type=jnp.float32,
                )
            xres[:, s * cols : (s + 1) * cols] = acc
        x = xres[...]
        mid = jnp.mean(x, axis=1, keepdims=True)
        dev = x - mid
        spread = jnp.mean(dev * dev, axis=1, keepdims=True)
        normed = (
            dev * (1.0 / jnp.sqrt(spread + EPS)) * ng_ref[l : l + 1, :] + ns_ref[l : l + 1, :]
        ).astype(jnp.bfloat16)
        for c in range(chunks):
            hid[c] = normed[:, c * cw : (c + 1) * cw]

    final = normed
    top = jnp.full((total, 1), -jnp.inf, jnp.float32)
    amount = jnp.zeros((total, 1), jnp.float32)
    pick = jnp.zeros((total, 1), jnp.float32)
    for v in range(vocab // wb):
        logits = lax.dot_general(
            final, emb[v * wb : (v + 1) * wb, :], nt, preferred_element_type=jnp.float32
        )
        words = lax.broadcasted_iota(jnp.int32, (total, wb), 1) + v * wb
        newer = jnp.maximum(top, jnp.max(logits, axis=1, keepdims=True))
        amount = amount * jnp.exp(top - newer) + jnp.sum(
            jnp.exp(logits - newer), axis=1, keepdims=True
        )
        pick = pick + jnp.sum(jnp.where(words == targets, logits, 0.0), axis=1, keepdims=True)
        top = newer
    diag = row_ids == col_ids

    def as_row(col):
        return jnp.sum(jnp.where(diag, col, 0.0), axis=0, keepdims=True)

    stats[0, 0:1, :] = as_row(top)
    stats[0, 1:2, :] = as_row(amount)
    stats[0, 2:3, :] = as_row(pick)
    stats[0, 3:8, :] = jnp.zeros((5, total), jnp.float32)
    st = [
        remote(stats.at[0], stats.at[k], st_s.at[k - 1], st_r.at[k - 1], seg_peer(k))
        for k in range(1, n)
    ]
    for copy in st:
        copy.start()
    for group in [id_copies] + rs_copies + w1_copies + w2_copies + w3_copies:
        for copy in group:
            copy.wait_send()
    for copy in st:
        copy.wait()
    best = stats[0, 0:1, :]
    for k in range(1, n):
        best = jnp.maximum(best, stats[k, 0:1, :])
    amount = jnp.zeros((1, total), jnp.float32)
    pick = jnp.zeros((1, total), jnp.float32)
    for k in range(n):
        amount = amount + stats[k, 1:2, :] * jnp.exp(stats[k, 0:1, :] - best)
        pick = pick + stats[k, 2:3, :]
    loglik = pick - (jnp.log(amount) + best)
    own = jnp.zeros((1, seg_len), jnp.float32)
    for s in range(n):
        own = own + jnp.where(me == s, 1.0, 0.0) * loglik[:, s * seg_len : (s + 1) * seg_len]
    row_out[...] = jnp.broadcast_to(own, row_out.shape)
    mean = jnp.sum(loglik, axis=1, keepdims=True) * (1.0 / total)
    mean_out[...] = jnp.broadcast_to(mean, mean_out.shape)


def hid_cols(hid, s, cols):
    cw = hid.shape[2]
    if cols == cw:
        return hid[s].astype(jnp.float32)
    c, at = divmod(s * cols, cw)
    return hid[c, :, at : at + cols].astype(jnp.float32)


def mega(
    n, docs, tokens, targets, embedding, qkv_weight, pos_weight, out_weight,
    content_bias, position_bias, norm_gain, norm_shift,
):
    seg_len = tokens.shape[0]
    vocab, width = embedding.shape
    layers = qkv_weight.shape[0]
    cols = width // n
    total = n * seg_len
    cw = 256
    chunks = width // cw
    pairs = docs // 2
    ids = jnp.broadcast_to(jnp.concatenate([tokens, targets])[None, :], (8, 2 * seg_len))
    qkv = qkv_weight.reshape(layers, width, 3 * cols)
    step = 16
    inverse = jnp.power(10000.0, -jnp.arange(0, width, 2).astype(jnp.float32) / width)[None, :]
    low = (step - 1 - jnp.arange(step)).astype(jnp.float32)[:, None] * inverse
    high = (total - step - step * jnp.arange(total // step)).astype(jnp.float32)[:, None] * inverse
    bf, f32 = jnp.bfloat16, jnp.float32
    dma = pltpu.SemaphoreType.DMA
    vmem = pl.BlockSpec(memory_space=pltpu.VMEM)
    hbm = pl.BlockSpec(memory_space=pl.ANY)
    row, mean = pl.pallas_call(
        functools.partial(
            mega_kernel, n, docs, seg_len, MEM_SEGS * seg_len, width // HEADS
        ),
        out_shape=(
            jax.ShapeDtypeStruct((8, seg_len), f32),
            jax.ShapeDtypeStruct((8, 128), f32),
        ),
        in_specs=[vmem, hbm, hbm, hbm, hbm] + [vmem] * 8,
        out_specs=(vmem, vmem),
        scratch_shapes=[
            pltpu.VMEM((vocab, width), bf),
            pltpu.VMEM((layers, width, 3 * cols), bf),
            pltpu.VMEM((layers, width, cols), bf),
            pltpu.VMEM((layers, n, width, cols), bf),
            pltpu.VMEM((n, 8, 2 * seg_len), jnp.int32),
            pltpu.VMEM((total, vocab), bf),
            pltpu.VMEM((chunks, total, cw), bf),
            pltpu.VMEM((chunks, n - 1, seg_len, cw), bf),
            pltpu.VMEM((chunks, total, cw), bf),
            pltpu.VMEM((total, width), bf),
            pltpu.VMEM((layers, total, cols), bf),
            pltpu.VMEM((layers, n, total, cols), bf),
            pltpu.VMEM((n, 8, total), f32),
            pltpu.VMEM((total, width), f32),
            dma((chunks,)), dma, dma, dma((layers,)),
            dma((n - 1,)), dma((n - 1,)),
            dma((chunks, n - 1)), dma((chunks, n - 1)),
            dma((chunks, n - 1)), dma((chunks, n - 1)),
            dma((layers, n - 1)), dma((layers, n - 1)),
            dma((layers, n - 1, pairs - 1)), dma((layers, n - 1, pairs - 1)),
            dma((layers, n - 1, pairs)), dma((layers, n - 1, pairs)),
            dma((layers, n - 1)), dma((layers, n - 1)),
            dma((n - 1,)), dma((n - 1,)),
        ],
        compiler_params=pltpu.CompilerParams(
            collective_id=0, has_side_effects=True, vmem_limit_bytes=60 * 1024 * 1024
        ),
    )(
        ids, embedding, qkv, pos_weight, out_weight, content_bias, position_bias,
        norm_gain, norm_shift, jnp.sin(low), jnp.cos(low), jnp.sin(high), jnp.cos(high),
    )
    return row[0], mean[0, :1]


def fits_kernel(n, docs, seg_len, vocab_rows, width, layers):
    cols = width // n
    total = n * seg_len
    return (
        n > 1 and docs >= 4 and docs % 2 == 0 and cols % 128 == 0 and 256 % cols == 0
        and width % 256 == 0 and vocab_rows % 512 == 0 and total % 128 == 0
        and 2 * seg_len == 128 and total <= 512 and width % docs == 0
        and (width // docs) % 16 == 0 and layers == 2
    )


def solution(mesh):
    in_specs = (
        P(("doc", "seg")),
        P(("doc", "seg")),
        P("seg", None),
        P(None, None, None, "seg"),
        P(None, None, "seg"),
        P(None, None, "seg"),
        P(),
        P(),
        P(),
        P(),
    )
    out_specs = (P(("doc", "seg")), P("doc"))
    n, docs = mesh.shape["seg"], mesh.shape["doc"]

    def body(tokens, targets, embedding, qkv_weight, *others):
        vocab_rows, width = embedding.shape
        layers = qkv_weight.shape[0]
        if fits_kernel(n, docs, tokens.shape[0], vocab_rows, width, layers):
            return mega(n, docs, tokens, targets, embedding, qkv_weight, *others)
        return on_device(tokens, targets, embedding, qkv_weight, *others)

    return jax.shard_map(
        body, mesh=mesh, in_specs=in_specs, out_specs=out_specs, check_vma=False
    )
```

```python
import functools
import math

import jax
import jax.numpy as jnp
from jax import lax
from jax.experimental import pallas as pl
from jax.experimental.pallas import tpu as pltpu
from jax.sharding import PartitionSpec as P

HEADS = 16
MEM_SEGS = 6
LAYERS = 2


def merged(shard, axis, combine):
    everything = jax.tree.map(lambda part: lax.all_gather(part, axis), shard)
    initial = jax.tree.map(lambda part: part[0], everything)

    def hop(k, so_far):
        return combine(so_far, jax.tree.map(lambda part: part[k], everything))

    return lax.fori_loop(1, lax.axis_size(axis), hop, initial)


def layer_norm(total, gain, shift):
    middle = jnp.mean(total, axis=-1, keepdims=True)
    spread = jnp.mean(jnp.square(total - middle), axis=-1, keepdims=True)
    return ((total - middle) / jnp.sqrt(spread + 1e-05) * gain + shift).astype(jnp.bfloat16)


def position_table(key_len, model_width):
    places = (key_len - 1 - jnp.arange(key_len)).astype(jnp.float32)
    inverse = jnp.power(10000.0, -jnp.arange(0, model_width, 2).astype(jnp.float32) / model_width)
    angles = places[:, None] * inverse[None, :]
    return jnp.concatenate([jnp.sin(angles), jnp.cos(angles)], axis=1).astype(jnp.bfloat16)


def relative_shift(raw_position, query_len, key_len):
    head_count = raw_position.shape[0]
    padded = jnp.pad(raw_position, ((0, 0), (0, 0), (0, 1)))
    flattened = padded.reshape(head_count, query_len * (key_len + 1))
    shifted = lax.slice_in_dim(
        flattened, query_len - 1, query_len - 1 + query_len * key_len, axis=1
    )
    return shifted.reshape(head_count, query_len, key_len)


def attend(with_content, with_position, key_heads, value_heads, pos_heads, visible, head_dim):
    query_len = with_content.shape[0]
    key_len = key_heads.shape[0]
    content = jnp.einsum(
        "thd,khd->htk", with_content, key_heads, preferred_element_type=jnp.float32
    )
    raw_position = jnp.einsum(
        "thd,khd->htk", with_position, pos_heads, preferred_element_type=jnp.float32
    )
    shifted = relative_shift(raw_position, query_len, key_len)
    scores = (content + shifted) * (1.0 / math.sqrt(head_dim))
    scores = jnp.where(visible[None], scores, jnp.float32(-1e30))
    row_max = jnp.max(scores, axis=2, keepdims=True)
    weights = jnp.exp(scores - row_max)
    attn_probs = (weights / jnp.sum(weights, axis=2, keepdims=True)).astype(jnp.bfloat16)
    head_mix = jnp.einsum(
        "htk,khd->thd", attn_probs, value_heads, preferred_element_type=jnp.float32
    )
    return head_mix.astype(jnp.bfloat16).reshape(query_len, with_content.shape[1] * head_dim)


def head_attention(layer_input, qkv_local, pos_local, u_row, v_row, head_dim):
    seg_len = layer_input.shape[0]
    model_width = layer_input.shape[1]
    group_size = lax.axis_size("seg")
    columns = qkv_local.shape[2]
    head_count = columns // head_dim
    mem_len = MEM_SEGS * seg_len
    first_column = lax.axis_index("seg") * columns
    matrix = qkv_local.reshape(model_width, 3 * columns)
    piece = lax.all_gather(layer_input, "seg", axis=0, tiled=True)
    product = jnp.dot(piece, matrix, preferred_element_type=jnp.float32)
    project = product.astype(jnp.bfloat16).reshape(piece.shape[0], 3, columns)
    total_rows = project.shape[0]
    block_segs = min(group_size, max(1, 512 // seg_len))
    while group_size % block_segs != 0:
        block_segs -= 1
    block_len = block_segs * seg_len
    key_span = mem_len + block_len
    block_count = group_size // block_segs
    pos_table = position_table(key_span, model_width)
    pos_keys = jnp.dot(pos_table, pos_local, preferred_element_type=jnp.float32).astype(
        jnp.bfloat16
    )
    pos_heads = pos_keys.reshape(key_span, head_count, head_dim)
    queries = project[:, 0, :].astype(jnp.float32)
    u_part = lax.dynamic_slice_in_dim(u_row, first_column, columns, 0)
    v_part = lax.dynamic_slice_in_dim(v_row, first_column, columns, 0)
    with_content = (queries + u_part).astype(jnp.bfloat16).reshape(total_rows, head_count, head_dim)
    with_position = (
        (queries + v_part).astype(jnp.bfloat16).reshape(total_rows, head_count, head_dim)
    )
    padded_kv = jnp.concatenate(
        [jnp.zeros((mem_len, 2, columns), jnp.bfloat16), project[:, 1:, :]], axis=0
    )
    row_ids = jnp.arange(block_len)[:, None]
    col_ids = jnp.arange(key_span)[None, :]

    def one_block(block_at):
        start = block_at * block_len
        block_content = lax.dynamic_slice_in_dim(with_content, start, block_len, 0)
        block_position = lax.dynamic_slice_in_dim(with_position, start, block_len, 0)
        window = lax.dynamic_slice_in_dim(padded_kv, start, key_span, 0)
        key_heads = window[:, 0, :].reshape(key_span, head_count, head_dim)
        value_heads = window[:, 1, :].reshape(key_span, head_count, head_dim)
        query_place = start + row_ids
        key_place = start - mem_len + col_ids
        visible = (key_place <= query_place) & (key_place >= 0)
        visible = visible & (key_place >= query_place // seg_len * seg_len - mem_len)
        return attend(
            block_content, block_position, key_heads, value_heads, pos_heads, visible, head_dim
        )

    mixed = lax.map(one_block, jnp.arange(block_count, dtype=jnp.int32)).reshape(
        total_rows, columns
    )
    return lax.all_to_all(mixed, "seg", split_axis=0, concat_axis=1, tiled=True)


def combine_words(first, second):
    top = jnp.maximum(first[0], second[0])
    total = first[1] * jnp.exp(first[0] - top) + second[1] * jnp.exp(second[0] - top)
    return (top, total, first[2] + second[2])


def on_device(
    tokens,
    targets,
    embedding,
    qkv_weight,
    pos_weight,
    out_weight,
    content_bias,
    position_bias,
    norm_gain,
    norm_shift,
):
    seg_len = tokens.shape[0]
    model_width = embedding.shape[1]
    vocab_rows = embedding.shape[0]
    head_dim = model_width // HEADS
    seg_index = lax.axis_index("seg")
    group_size = lax.axis_size("seg")
    first_word = seg_index * vocab_rows
    all_tokens, all_targets = (
        lax.all_gather(tokens, "seg", axis=0, tiled=True),
        lax.all_gather(targets, "seg", axis=0, tiled=True),
    )
    local_ids = all_tokens - first_word
    inside = (local_ids >= 0) & (local_ids < vocab_rows)
    rows = jnp.take(embedding, jnp.clip(local_ids, 0, vocab_rows - 1), axis=0)
    looked = lax.psum_scatter(
        jnp.where(inside[:, None], rows.astype(jnp.float32), 0.0).astype(jnp.bfloat16),
        "seg",
        scatter_dimension=0,
        tiled=True,
    ).astype(jnp.float32)
    hidden = (looked * math.sqrt(model_width)).astype(jnp.bfloat16)
    for layer_at in range(LAYERS):
        layer_input = hidden
        head_mix = head_attention(
            layer_input,
            qkv_weight[layer_at],
            pos_weight[layer_at],
            content_bias[layer_at],
            position_bias[layer_at],
            head_dim,
        )
        attended = jnp.dot(
            head_mix,
            lax.all_gather(out_weight[layer_at], "seg", axis=1, tiled=True),
            preferred_element_type=jnp.float32,
        )
        hidden = layer_norm(
            layer_input.astype(jnp.float32) + attended, norm_gain[layer_at], norm_shift[layer_at]
        )
    word_ids = first_word + jnp.arange(vocab_rows)[None, :]
    logits = jnp.einsum(
        "td,vd->tv",
        lax.all_gather(hidden, "seg", axis=0, tiled=True),
        embedding,
        preferred_element_type=jnp.float32,
    )
    piece_max = jnp.max(logits, axis=1)
    piece_sum = jnp.sum(jnp.exp(logits - piece_max[:, None]), axis=1)
    piece_pick = jnp.sum(jnp.where(word_ids == all_targets[:, None], logits, 0.0), axis=1)
    top, total, picked = merged((piece_max, piece_sum, piece_pick), "seg", combine_words)
    own_start = seg_index * seg_len
    own_top = lax.dynamic_slice_in_dim(top, own_start, seg_len, 0)
    own_total = lax.dynamic_slice_in_dim(total, own_start, seg_len, 0)
    own_pick = lax.dynamic_slice_in_dim(picked, own_start, seg_len, 0)
    token_loglik = own_pick - (jnp.log(own_total) + own_top)
    grand_total = lax.psum(jnp.sum(token_loglik), "seg")
    doc_mean = (grand_total / (seg_len * group_size)).reshape(1)
    return (token_loglik, doc_mean)


MESH = pl.DeviceIdType.MESH
EPS = 1e-05


def mega_kernel(
    n, docs, seg_len, mem_len, head_dim,
    tokens_ref, targets_ref, emb_hbm, qkv_hbm, pos_hbm, out_hbm, cb_ref, pb_ref, ng_ref, ns_ref,
    lo_sin, lo_cos, hi_sin, hi_cos,
    row_out, mean_out,
    emb, qkv, posw, wfull, idbuf, onehot, gsend, fromleft, fromright, toright, toleft, hid, table, pkeys, mixg, stats, xres,
    emb_sem, w_sem, p_sem, o_sem,
    id_s, id_r, rr_s, rr_r, rl_s, rl_r, w1_s, w1_r, w2_s, w2_r, w3_s, w3_r, mr_s, mr_r, ml_s, ml_r, st_s, st_r,
):
    layers = qkv.shape[0]
    total = n * seg_len
    vocab, width = emb.shape
    cols = width // n
    chunks = hid.shape[0]
    cw = hid.shape[2]
    per = width // docs
    me = lax.axis_index("seg")
    doc = lax.axis_index("doc")
    pairs = docs // 2
    core = lax.rem(doc, 2)
    chip = doc // 2
    partner = chip * 2 + 1 - core

    def seg_peer(k):
        return (doc, lax.rem(me + k, n))

    def plane_peer(j):
        return (lax.rem(chip + j, pairs) * 2 + core, me)

    def remote(src, dst, send, recv, device):
        return pltpu.make_async_remote_copy(
            src_ref=src, dst_ref=dst, send_sem=send, recv_sem=recv,
            device_id=device, device_id_type=MESH,
        )

    emb_copies = [
        pltpu.make_async_copy(
            emb_hbm.at[:, c * cw : (c + 1) * cw], emb.at[:, c * cw : (c + 1) * cw], emb_sem.at[c]
        )
        for c in range(chunks)
    ]
    out_copies = [
        pltpu.make_async_copy(out_hbm.at[l], wfull.at[l, me], o_sem.at[l]) for l in range(layers)
    ]
    pos_copy = pltpu.make_async_copy(pos_hbm, posw, p_sem)
    qkv_copy = pltpu.make_async_copy(qkv_hbm, qkv, w_sem)
    out_copies[0].start()
    emb_copies[0].start()
    for copy in emb_copies[1:]:
        copy.start()
    for copy in out_copies[1:]:
        copy.start()
    pos_copy.start()
    qkv_copy.start()

    idbuf[n - 1, 0:1, :seg_len] = tokens_ref[...]
    idbuf[n - 1, 0:1, seg_len:] = targets_ref[...]
    idbuf[n - 1, 1:8, :] = jnp.zeros((7, 2 * seg_len), jnp.int32)
    barrier = pltpu.get_barrier_semaphore()
    friends = [seg_peer(k) for k in range(1, n)] + [plane_peer(j) for j in range(1, pairs)]
    friends.append((partner, me))
    for friend in friends:
        pl.semaphore_signal(barrier, inc=1, device_id=friend, device_id_type=MESH)
    pl.semaphore_wait(barrier, len(friends))

    id_copies = [
        remote(idbuf.at[n - 1], idbuf.at[k - 1], id_s.at[k - 1], id_r.at[k - 1], seg_peer(k))
        for k in range(1, n)
    ]
    for copy in id_copies:
        copy.start()

    mine = pl.ds(pl.multiple_of(doc * per, per), per)

    def w1(l):
        return [
            remote(
                out_hbm.at[l, mine], wfull.at[l, me, mine], w1_s.at[l, k - 1],
                w1_r.at[l, k - 1], seg_peer(k),
            )
            for k in range(1, n)
        ]

    w1_copies = [w1(l) for l in range(layers)]
    for copy in w1_copies[0]:
        copy.start()

    def w2(l):
        found = []
        for k in range(1, n):
            src = lax.rem(me - k + n, n)
            for j in range(1, pairs):
                ref = wfull.at[l, src, mine]
                found.append(
                    remote(ref, ref, w2_s.at[l, k - 1, j - 1], w2_r.at[l, k - 1, j - 1], plane_peer(j))
                )
        return found

    def w3(l):
        found = []
        for k in range(1, n):
            src = lax.rem(me - k + n, n)
            for j in range(pairs):
                owner = lax.rem(chip - j + pairs, pairs) * 2 + core
                ref = wfull.at[l, src, pl.ds(pl.multiple_of(owner * per, per), per)]
                found.append(
                    remote(ref, ref, w3_s.at[l, k - 1, j], w3_r.at[l, k - 1, j], (partner, me))
                )
        return found

    w2_copies = [w2(l) for l in range(layers)]
    w3_copies = [w3(l) for l in range(layers)]

    eye = lax.broadcasted_iota(jnp.int32, (2 * seg_len, 2 * seg_len), 0) == lax.broadcasted_iota(
        jnp.int32, (2 * seg_len, 2 * seg_len), 1
    )

    def column(row):
        return jnp.sum(jnp.where(eye, row, 0), axis=1, keepdims=True)

    for copy in id_copies:
        copy.wait_recv()
    first_word = me * vocab
    tok_cols = []
    tgt_cols = []
    for s in range(n):
        slot = lax.rem(me - s + 2 * n - 1, n)
        both = column(idbuf[slot, 0:1, :]) - first_word
        tok_cols.append(both[:seg_len])
        tgt_cols.append(both[seg_len:])
    tokens = jnp.concatenate(tok_cols, axis=0)
    targets = jnp.concatenate(tgt_cols, axis=0)
    wb = 512
    for v in range(vocab // wb):
        words = lax.broadcasted_iota(jnp.int32, (total, wb), 1) + v * wb
        onehot[:, v * wb : (v + 1) * wb] = (tokens == words).astype(jnp.float32).astype(jnp.bfloat16)

    def rows_of(s):
        return pl.ds(pl.multiple_of(s * seg_len, seg_len), seg_len)

    steps = gsend.shape[0]
    nw = gsend.shape[2]
    right = (doc, jnp.minimum(me + 1, n - 1))
    left = (doc, jnp.maximum(me - 1, 0))

    @pl.when(me == 0)
    def _():
        fromleft[...] = jnp.zeros_like(fromleft)

    @pl.when(me == n - 1)
    def _():
        fromright[...] = jnp.zeros_like(fromright)

    def chain_right(c):
        return remote(toright.at[c], fromleft.at[c], rr_s.at[c], rr_r.at[c], right)

    def chain_left(c):
        return remote(toleft.at[c], fromright.at[c], rl_s.at[c], rl_r.at[c], left)

    def advance(t):
        cr = t - me

        @pl.when((cr >= 0) & (cr < steps))
        def _():
            @pl.when(me > 0)
            def _():
                chain_right(cr).wait_recv()

            @pl.when(me < n - 1)
            def _():
                toright[cr] = fromleft[cr] + gsend[cr]
                chain_right(cr).start()

        cl = t - (n - 1 - me)

        @pl.when((cl >= 0) & (cl < steps))
        def _():
            @pl.when(me < n - 1)
            def _():
                chain_left(cl).wait_recv()

            @pl.when(me > 0)
            def _():
                toleft[cl] = fromright[cl] + gsend[cl]
                chain_left(cl).start()

    for c in range(steps):
        if c * nw % cw == 0:
            emb_copies[c * nw // cw].wait()
        gsend[c] = jnp.dot(
            onehot[...], emb[:, c * nw : (c + 1) * nw], preferred_element_type=jnp.float32
        ).astype(jnp.bfloat16)
        advance(c)

    for copy in w1_copies[0]:
        copy.wait_recv()
    for copy in w2_copies[0]:
        copy.start()

    step = lo_sin.shape[0]
    half = width // 2
    for a in range(total // step):
        hs = hi_sin[a : a + 1, :]
        hc = hi_cos[a : a + 1, :]
        rows = slice(a * step, (a + 1) * step)
        table[rows, :half] = (hs * lo_cos[...] + hc * lo_sin[...]).astype(jnp.bfloat16)
        table[rows, half:] = (hc * lo_cos[...] - hs * lo_sin[...]).astype(jnp.bfloat16)

    pl.loop(steps, steps + n - 1)(advance)
    for l in range(1, layers):
        for copy in w1_copies[l]:
            copy.start()

    pos_copy.wait()
    for l in range(layers):
        pkeys[l] = jnp.dot(table[...], posw[l], preferred_element_type=jnp.float32).astype(
            jnp.bfloat16
        )
    for copy in w2_copies[0]:
        copy.wait_recv()
    for copy in w3_copies[0]:
        copy.start()
    qkv_copy.wait()
    for c in range(steps):
        looked = fromleft[c].astype(jnp.float32) + gsend[c].astype(jnp.float32)
        looked = (looked + fromright[c].astype(jnp.float32)) * math.sqrt(width)
        at = c * nw % cw
        hid[c * nw // cw, :, at : at + nw] = looked.astype(jnp.bfloat16)

    def move_right(l, j, b, src):
        ref = mixg.at[l, jnp.maximum(src, 0), b * rb : (b + 1) * rb]
        return remote(ref, ref, mr_s.at[l, j, b], mr_r.at[l, j, b], right)

    def move_left(l, j, b, src):
        ref = mixg.at[l, jnp.minimum(src, n - 1), b * rb : (b + 1) * rb]
        return remote(ref, ref, ml_s.at[l, j, b], ml_r.at[l, j, b], left)

    def each_way(l, j, b, part):
        if part == "start" or part == "sent":
            act_r = (me - j >= 0) & (me < n - 1)
            act_l = (me + j < n) & (me > 0)
            at_r, at_l = me - j, me + j
        else:
            act_r = me - 1 - j >= 0
            act_l = me + 1 + j < n
            at_r, at_l = me - 1 - j, me + 1 + j

        def act(copy):
            if part == "start":
                copy.start()
            elif part == "sent":
                copy.wait_send()
            else:
                copy.wait_recv()

        @pl.when(act_r)
        def _():
            act(move_right(l, j, b, at_r))

        @pl.when(act_l)
        def _():
            act(move_left(l, j, b, at_l))

    halves = mr_s.shape[2]
    rb = total // halves
    row_ids = lax.broadcasted_iota(jnp.int32, (total, total), 0)
    col_ids = lax.broadcasted_iota(jnp.int32, (total, total), 1)
    seg_start = row_ids // seg_len * seg_len
    visible = (col_ids <= row_ids) & (col_ids >= seg_start - mem_len)
    lanes = lax.broadcasted_iota(jnp.int32, (1, cols), 1) // head_dim
    heads = cols // head_dim
    own_cols = pl.ds(pl.multiple_of(me * cols, cols), cols)
    nt = (((1,), (1,)), ((), ()))

    for l in range(layers):
        parts = []
        for j in range(3):
            acc = None
            for c in range(chunks):
                term = jnp.dot(
                    hid[c], qkv[l, j, c * cw : (c + 1) * cw, :],
                    preferred_element_type=jnp.float32,
                )
                acc = term if acc is None else acc + term
            parts.append(acc.astype(jnp.bfloat16))
        query, key, value = parts
        query = query.astype(jnp.float32)
        content_q = query + cb_ref[l : l + 1, own_cols]
        position_q = query + pb_ref[l : l + 1, own_cols]
        for b in range(halves):
            rows = slice(b * rb, (b + 1) * rb)
            span = (b + 1) * rb
            mixed = jnp.zeros((rb, cols), jnp.float32)
            for h in range(heads):
                here = lanes == h
                cq = jnp.where(here, content_q[rows], 0.0).astype(jnp.bfloat16)
                pq = jnp.where(here, position_q[rows], 0.0).astype(jnp.bfloat16)
                content = lax.dot_general(cq, key[:span], nt, preferred_element_type=jnp.float32)
                raw = lax.dot_general(pq, pkeys[l], nt, preferred_element_type=jnp.float32)
                shifted = pltpu.roll(raw, b * rb + 1, 1, stride=1, stride_axis=0)[:, :span]
                scores = (content + shifted) * (1.0 / math.sqrt(head_dim))
                scores = jnp.where(visible[rows, :span], scores, -1e30)
                top = jnp.max(scores, axis=1, keepdims=True)
                weights = jnp.exp(scores - top)
                probs = (weights * (1.0 / jnp.sum(weights, axis=1, keepdims=True))).astype(
                    jnp.bfloat16
                )
                out = jnp.dot(probs, value[:span], preferred_element_type=jnp.float32)
                mixed = jnp.where(here, out, mixed)
            mixg[l, me, rows, :] = mixed.astype(jnp.bfloat16)
            each_way(l, 0, b, "start")
        for j in range(1, n - 1):
            for b in range(halves):
                each_way(l, j - 1, b, "got")
                each_way(l, j, b, "start")
        if l + 1 < layers:
            for copy in w1_copies[l + 1]:
                copy.wait_recv()
            for copy in w2_copies[l + 1]:
                copy.start()
        if l > 0:
            for copy in w2_copies[l]:
                copy.wait_recv()
            for copy in w3_copies[l]:
                copy.start()
        for copy in w3_copies[l]:
            copy.wait_recv()
        out_copies[l].wait()
        normed = []
        for b in range(halves):
            rows = slice(b * rb, (b + 1) * rb)
            each_way(l, n - 2, b, "got")
            for s in range(n):
                acc = hid_cols(hid, s, cols)[rows]
                for k in range(n):
                    acc = acc + jnp.dot(
                        mixg[l, k, rows, :], wfull[l, s, k * cols : (k + 1) * cols, :],
                        preferred_element_type=jnp.float32,
                    )
                xres[rows, s * cols : (s + 1) * cols] = acc
            x = xres[rows, :]
            mid = jnp.mean(x, axis=1, keepdims=True)
            dev = x - mid
            spread = jnp.mean(dev * dev, axis=1, keepdims=True)
            normed.append(
                (
                    dev * (1.0 / jnp.sqrt(spread + EPS)) * ng_ref[l : l + 1, :]
                    + ns_ref[l : l + 1, :]
                ).astype(jnp.bfloat16)
            )
        normed = jnp.concatenate(normed, axis=0)
        for c in range(chunks):
            hid[c] = normed[:, c * cw : (c + 1) * cw]

    final = normed
    top = jnp.full((total, 1), -jnp.inf, jnp.float32)
    amount = jnp.zeros((total, 1), jnp.float32)
    pick = jnp.zeros((total, 1), jnp.float32)
    for v in range(vocab // wb):
        logits = lax.dot_general(
            final, emb[v * wb : (v + 1) * wb, :], nt, preferred_element_type=jnp.float32
        )
        words = lax.broadcasted_iota(jnp.int32, (total, wb), 1) + v * wb
        newer = jnp.maximum(top, jnp.max(logits, axis=1, keepdims=True))
        amount = amount * jnp.exp(top - newer) + jnp.sum(
            jnp.exp(logits - newer), axis=1, keepdims=True
        )
        pick = pick + jnp.sum(jnp.where(words == targets, logits, 0.0), axis=1, keepdims=True)
        top = newer
    diag = row_ids == col_ids

    def as_row(col):
        return jnp.sum(jnp.where(diag, col, 0.0), axis=0, keepdims=True)

    stats[0, 0:1, :] = as_row(top)
    stats[0, 1:2, :] = as_row(amount)
    stats[0, 2:3, :] = as_row(pick)
    stats[0, 3:8, :] = jnp.zeros((5, total), jnp.float32)
    st = [
        remote(stats.at[0], stats.at[k], st_s.at[k - 1], st_r.at[k - 1], seg_peer(k))
        for k in range(1, n)
    ]
    for copy in st:
        copy.start()
    for c in range(steps):
        @pl.when(me < n - 1)
        def _():
            chain_right(c).wait_send()

        @pl.when(me > 0)
        def _():
            chain_left(c).wait_send()

    for l in range(layers):
        for j in range(n - 1):
            for b in range(halves):
                each_way(l, j, b, "sent")
    for group in [id_copies] + w1_copies + w2_copies + w3_copies:
        for copy in group:
            copy.wait_send()
    for copy in st:
        copy.wait()
    best = stats[0, 0:1, :]
    for k in range(1, n):
        best = jnp.maximum(best, stats[k, 0:1, :])
    amount = jnp.zeros((1, total), jnp.float32)
    pick = jnp.zeros((1, total), jnp.float32)
    for k in range(n):
        amount = amount + stats[k, 1:2, :] * jnp.exp(stats[k, 0:1, :] - best)
        pick = pick + stats[k, 2:3, :]
    loglik = pick - (jnp.log(amount) + best)
    own = jnp.zeros((1, seg_len), jnp.float32)
    for s in range(n):
        own = own + jnp.where(me == s, 1.0, 0.0) * loglik[:, s * seg_len : (s + 1) * seg_len]
    row_out[...] = own
    mean = jnp.sum(loglik, axis=1, keepdims=True) * (1.0 / total)
    mean_out[...] = mean


def hid_cols(hid, s, cols):
    cw = hid.shape[2]
    if cols == cw:
        return hid[s].astype(jnp.float32)
    c, at = divmod(s * cols, cw)
    return hid[c, :, at : at + cols].astype(jnp.float32)


def mega(
    n, docs, tokens, targets, embedding, qkv_weight, pos_weight, out_weight,
    content_bias, position_bias, norm_gain, norm_shift,
):
    seg_len = tokens.shape[0]
    vocab, width = embedding.shape
    layers = qkv_weight.shape[0]
    cols = width // n
    total = n * seg_len
    cw = 256
    chunks = width // cw
    nw = 128
    steps = width // nw
    pairs = docs // 2
    qkv = qkv_weight.transpose(0, 2, 1, 3)
    step = 16
    inverse = jnp.power(10000.0, -jnp.arange(0, width, 2).astype(jnp.float32) / width)[None, :]
    low = (step - 1 - jnp.arange(step)).astype(jnp.float32)[:, None] * inverse
    high = (total - step - step * jnp.arange(total // step)).astype(jnp.float32)[:, None] * inverse
    bf, f32 = jnp.bfloat16, jnp.float32
    dma = pltpu.SemaphoreType.DMA
    vmem = pl.BlockSpec(memory_space=pltpu.VMEM)
    hbm = pl.BlockSpec(memory_space=pl.ANY)
    row, mean = pl.pallas_call(
        functools.partial(
            mega_kernel, n, docs, seg_len, MEM_SEGS * seg_len, width // HEADS
        ),
        out_shape=(
            jax.ShapeDtypeStruct((1, seg_len), f32),
            jax.ShapeDtypeStruct((1, 1), f32),
        ),
        in_specs=[vmem] * 2 + [hbm] * 4 + [vmem] * 8,
        out_specs=(vmem, vmem),
        scratch_shapes=[
            pltpu.VMEM((vocab, width), bf),
            pltpu.VMEM((layers, 3, width, cols), bf),
            pltpu.VMEM((layers, width, cols), bf),
            pltpu.VMEM((layers, n, width, cols), bf),
            pltpu.VMEM((n, 8, 2 * seg_len), jnp.int32),
            pltpu.VMEM((total, vocab), bf),
            pltpu.VMEM((steps, total, nw), bf),
            pltpu.VMEM((steps, total, nw), bf),
            pltpu.VMEM((steps, total, nw), bf),
            pltpu.VMEM((steps, total, nw), bf),
            pltpu.VMEM((steps, total, nw), bf),
            pltpu.VMEM((chunks, total, cw), bf),
            pltpu.VMEM((total, width), bf),
            pltpu.VMEM((layers, total, cols), bf),
            pltpu.VMEM((layers, n, total, cols), bf),
            pltpu.VMEM((n, 8, total), f32),
            pltpu.VMEM((total, width), f32),
            dma((chunks,)), dma, dma, dma((layers,)),
            dma((n - 1,)), dma((n - 1,)),
            dma((steps,)), dma((steps,)), dma((steps,)), dma((steps,)),
            dma((layers, n - 1)), dma((layers, n - 1)),
            dma((layers, n - 1, pairs - 1)), dma((layers, n - 1, pairs - 1)),
            dma((layers, n - 1, pairs)), dma((layers, n - 1, pairs)),
            dma((layers, n - 1, 2)), dma((layers, n - 1, 2)),
            dma((layers, n - 1, 2)), dma((layers, n - 1, 2)),
            dma((n - 1,)), dma((n - 1,)),
        ],
        compiler_params=pltpu.CompilerParams(
            collective_id=0, has_side_effects=True, vmem_limit_bytes=60 * 1024 * 1024
        ),
    )(
        tokens[None, :], targets[None, :], embedding, qkv, pos_weight, out_weight, content_bias, position_bias,
        norm_gain, norm_shift, jnp.sin(low), jnp.cos(low), jnp.sin(high), jnp.cos(high),
    )
    return row.reshape(seg_len), mean.reshape(1)


def fits_kernel(n, docs, seg_len, vocab_rows, width, layers):
    cols = width // n
    total = n * seg_len
    return (
        n > 1 and docs >= 4 and docs % 2 == 0 and cols % 128 == 0 and 256 % cols == 0
        and width % 256 == 0 and vocab_rows % 512 == 0 and total % 128 == 0
        and 2 * seg_len == 128 and total <= 512 and width % docs == 0
        and (width // docs) % 16 == 0 and layers == 2
    )


def solution(mesh):
    in_specs = (
        P(("doc", "seg")),
        P(("doc", "seg")),
        P("seg", None),
        P(None, None, None, "seg"),
        P(None, None, "seg"),
        P(None, None, "seg"),
        P(),
        P(),
        P(),
        P(),
    )
    out_specs = (P(("doc", "seg")), P("doc"))
    n, docs = mesh.shape["seg"], mesh.shape["doc"]

    def body(tokens, targets, embedding, qkv_weight, *others):
        vocab_rows, width = embedding.shape
        layers = qkv_weight.shape[0]
        if fits_kernel(n, docs, tokens.shape[0], vocab_rows, width, layers):
            return mega(n, docs, tokens, targets, embedding, qkv_weight, *others)
        return on_device(tokens, targets, embedding, qkv_weight, *others)

    return jax.shard_map(
        body, mesh=mesh, in_specs=in_specs, out_specs=out_specs, check_vma=False
    )
```
